32 devices in a mesh: inter: 16 (over z, y, core), intra: 2 (over x).
Axes of the slice: x: 2, y: 2, z: 4, core: 2. Of those that a mesh axis runs over, the one named last changes fastest.
Arguments:
- hidden_in: bfloat16 [16, 256, 4096], P('inter', 'intra'), may hold values from -120 to 120, as said below
- norm_gain: bfloat16 [4096], P(('inter', 'intra')), may hold values from 0.5 to 2, as said below
- qkv_weight: bfloat16 [4096, 768], P(('inter', 'intra')), may hold values from -0.09375 to 0.09375
- attn_cotangent: bfloat16 [16, 256, 512], P('inter', 'intra'), may hold values from -6 to 6
Outputs:
- attn: bfloat16 [16, 256, 512], P('inter', 'intra')
- grad_in: bfloat16 [16, 256, 4096], P('inter', 'intra')
- weight_grad: float32 [4096, 768], P(('intra', 'inter'))
- gain_grad: float32 [4096], P(('intra', 'inter'))
The draws below stay inside these ranges and needn't reach their ends.
Inputs may be any that keep to these rules, and one draw needn't show every extreme that they name: `hidden_in`: activations with spread row and feature scales. `norm_gain`: positive gains.
All inputs are finite; a program needn't handle non-finite values.
Results may differ from the reference program's by a relative error of at most 0.015.
Values may be sent and summed in bfloat16 or wider, within the bound.
A program may use at most 64 MiB of HBM per device.

```python
import math
import jax
import jax.numpy as jnp
from jax import lax

D = 4096
HD = 128
HEADS = 4
SEQ = 256
SEQS = 16


def draw_hidden_in(key, part):
    key_base, key_rows, key_cols = jax.random.split(jax.random.fold_in(key, 11), 3)
    shape = (SEQS, SEQ, D)
    row_scale = jnp.exp(jax.random.uniform(key_rows, (SEQS, SEQ, 1), minval=0.0, maxval=math.log(10.0)))
    col_scale = jnp.exp(jax.random.uniform(key_cols, (1, 1, D), minval=math.log(0.5), maxval=math.log(3.0)))
    base = jnp.clip(jax.random.normal(key_base, shape), -4.0, 4.0)
    return (base * row_scale * col_scale).astype(jnp.bfloat16)


def draw_norm_gain(key, part):
    key_gain = jax.random.fold_in(key, 23)
    values_out = jnp.exp(jax.random.uniform(key_gain, (D,), minval=math.log(0.5), maxval=math.log(2.0)))
    return values_out.astype(jnp.bfloat16)


def block_scale(key, shape, cuts, least, high):
    loudness, own = 1.0, jax.random.fold_in(key, 6)
    for position, blocks in cuts:
        draws = jnp.exp(jax.random.uniform(jax.random.fold_in(own, position), (blocks,), jnp.float32, least / len(cuts), high / len(cuts)))
        loudness = loudness * jnp.repeat(draws, shape[position] // blocks).reshape([-1 if axis == position else 1 for axis in range(len(shape))])
    return loudness


def centred(stream_key, extent, width, bound, pieces=(), held_as=jnp.bfloat16):
    entries = width * jax.random.normal(stream_key, extent, jnp.float32)
    if pieces:
        entries = entries * block_scale(stream_key, extent, pieces, -0.22, 0.18)
    return jnp.clip(entries, -bound, bound).astype(held_as)


def setup_inputs(seed: int = 0) -> dict:
    arg_keys = jax.random.split(jax.random.key(seed), 5)
    return {
        "hidden_in": draw_hidden_in(jax.random.fold_in(arg_keys[4], 71), 0),
        "norm_gain": draw_norm_gain(jax.random.fold_in(arg_keys[4], 71), 0),
        "qkv_weight": centred(arg_keys[2], (D, (HEADS + 2) * HD), D ** -0.5, 0.09375, ((0, 32),)),
        "attn_cotangent": centred(arg_keys[3], (SEQS, SEQ, HEADS * HD), 1.0, 6.0, ((0, 16), (1, 2))),
    }


eps_norm = 1e-05
rope_base = 500000.0

def rope_tables(positions, head_size):
    half_size = head_size // 2
    freqs = rope_base ** (-jnp.arange(half_size, dtype=jnp.float32) / half_size)
    angles = positions.astype(jnp.float32)[:, None] * freqs[None, :]
    return (jnp.cos(angles), jnp.sin(angles))

def rotate(values_in, cosine, sine):
    half_size = values_in.shape[-1] // 2
    first, second = (values_in[..., :half_size], values_in[..., half_size:])
    return jnp.concatenate([first * cosine - second * sine, second * cosine + first * sine], axis=-1)

def unrotate(grad_out, cosine, sine):
    half_size = grad_out.shape[-1] // 2
    first, second = (grad_out[..., :half_size], grad_out[..., half_size:])
    return jnp.concatenate([first * cosine + second * sine, second * cosine - first * sine], axis=-1)

def reference(hidden_in, norm_gain, qkv_weight, attn_cotangent):
    gain = norm_gain.astype(jnp.float32)
    positions = jnp.arange(SEQ, dtype=jnp.int32)
    cosine, sine = rope_tables(positions, HD)
    row_pos = jnp.arange(SEQ * HEADS, dtype=jnp.int32) // HEADS
    allowed = positions[None, :] <= row_pos[:, None]
    scale = HD ** (-0.5)
    qcols = HEADS * HD

    def one_sequence(carry, items):
        weight_acc, gain_acc = carry
        rows_in, grad_attn = items
        wide_rows = rows_in.astype(jnp.float32)
        inv_rms = lax.rsqrt(lax.optimization_barrier(jnp.mean(wide_rows * wide_rows, axis=1, keepdims=True)) + eps_norm)
        normed = (wide_rows * inv_rms * gain[None, :]).astype(jnp.bfloat16)
        mixed = jnp.dot(normed, qkv_weight, preferred_element_type=jnp.float32)
        query = (rotate(mixed[:, :qcols].reshape(SEQ, HEADS, HD), cosine[:, None, :], sine[:, None, :]) * scale).astype(jnp.bfloat16).reshape(SEQ * HEADS, HD)
        key_rows = rotate(mixed[:, qcols:qcols + HD], cosine, sine).astype(jnp.bfloat16)
        value_rows = mixed[:, qcols + HD:].astype(jnp.bfloat16)
        grad_flat = grad_attn.reshape(SEQ * HEADS, HD)
        scores = jnp.dot(query, key_rows.T, preferred_element_type=jnp.float32)
        scores = jnp.where(allowed, scores, -1e+30)
        row_top = lax.optimization_barrier(jnp.max(scores, axis=1))
        row_total = lax.optimization_barrier(jnp.sum(jnp.where(allowed, jnp.exp(scores - row_top[:, None]), 0.0), axis=1))
        log_total = row_top + jnp.log(row_total)
        probs = jnp.where(allowed, jnp.exp(scores - log_total[:, None]), 0.0)
        probs_low = probs.astype(jnp.bfloat16)
        attn_flat = jnp.dot(probs, value_rows.astype(jnp.float32), precision=lax.Precision.HIGHEST, preferred_element_type=jnp.float32).astype(jnp.bfloat16)
        row_delta = lax.optimization_barrier(jnp.sum(grad_flat.astype(jnp.float32) * attn_flat.astype(jnp.float32), axis=1))
        grad_probs = jnp.dot(grad_flat, value_rows.T, preferred_element_type=jnp.float32)
        grad_scores = (probs * (grad_probs - row_delta[:, None])).astype(jnp.bfloat16)
        grad_query = jnp.dot(grad_scores, key_rows, preferred_element_type=jnp.float32)
        grad_keys = jnp.dot(grad_scores.T, query, preferred_element_type=jnp.float32)
        grad_values = jnp.dot(probs_low.T, grad_flat, preferred_element_type=jnp.float32)
        query_back = (unrotate(grad_query.reshape(SEQ, HEADS, HD), cosine[:, None, :], sine[:, None, :]) * scale).reshape(SEQ, qcols)
        grad_mixed = jnp.concatenate([query_back, unrotate(grad_keys, cosine, sine), grad_values], axis=1).astype(jnp.bfloat16)
        grad_normed = jnp.dot(grad_mixed, qkv_weight.T, preferred_element_type=jnp.float32)
        inner = lax.optimization_barrier(jnp.sum(grad_normed * gain[None, :] * wide_rows, axis=1, keepdims=True))
        grad_rows = (gain[None, :] * grad_normed * inv_rms - wide_rows * inv_rms ** 3 / D * inner).astype(jnp.bfloat16)
        gain_acc = gain_acc + lax.optimization_barrier(jnp.sum(grad_normed * wide_rows * inv_rms, axis=0))
        term_low = jnp.dot(normed.T, grad_mixed, preferred_element_type=jnp.float32).astype(jnp.bfloat16)
        term_low = lax.optimization_barrier(term_low)
        weight_acc = weight_acc + term_low.astype(jnp.float32)
        return ((weight_acc, gain_acc), (attn_flat.reshape(SEQ, qcols), grad_rows))
    start = (jnp.zeros((D, (HEADS + 2) * HD), jnp.float32), jnp.zeros((D,), jnp.float32))
    (weight_grad, gain_grad), (attn, grad_in) = lax.scan(one_sequence, start, (hidden_in, attn_cotangent))
    return (attn, grad_in, weight_grad, gain_grad)
```

```python
import functools
import jax
import jax.numpy as jnp
import numpy as np
from jax import lax
from jax.experimental import pallas as pl
from jax.experimental.pallas import tpu as pltpu
from jax.sharding import PartitionSpec as P

HD = 128
HEADS = 4


eps_norm = 1e-05
rope_base = 500000.0


def rope_tables(positions, head_size):
    half_size = head_size // 2
    freqs = rope_base ** (-jnp.arange(half_size, dtype=jnp.float32) / half_size)
    angles = positions.astype(jnp.float32)[:, None] * freqs[None, :]
    return (jnp.cos(angles), jnp.sin(angles))


def rotate(values_in, cosine, sine):
    half_size = values_in.shape[-1] // 2
    first, second = (values_in[..., :half_size], values_in[..., half_size:])
    return jnp.concatenate(
        [first * cosine - second * sine, second * cosine + first * sine], axis=-1
    )


def unrotate(grad_out, cosine, sine):
    half_size = grad_out.shape[-1] // 2
    first, second = (grad_out[..., :half_size], grad_out[..., half_size:])
    return jnp.concatenate(
        [first * cosine + second * sine, second * cosine - first * sine], axis=-1
    )


def forward_fold(query_rows, row_pos):

    def forward_advance(carry, piece, start):
        row_top, row_total, weighted = carry
        key_part, value_part = piece
        scores = jnp.einsum("qd,kd->qk", query_rows, key_part, preferred_element_type=jnp.float32)
        key_pos = jnp.arange(key_part.shape[0], dtype=jnp.int32)
        allowed = key_pos[None, :] <= row_pos[:, None]
        scores = jnp.where(allowed, scores, -1e30)
        new_top = jnp.maximum(row_top, jnp.max(scores, axis=1))
        numbers = jnp.where(allowed, jnp.exp(scores - new_top[:, None]), 0.0)
        row_total = jnp.sum(numbers, axis=1)
        weighted = jnp.dot(
            numbers,
            value_part.astype(jnp.float32),
            precision=lax.Precision.HIGHEST,
            preferred_element_type=jnp.float32,
        )
        return (new_top, row_total, weighted)

    return forward_advance


def query_grad_fold(query_rows, row_pos, grad_flat, log_total, row_delta):

    def query_advance(grad_query, piece, start):
        key_part, value_part = piece
        scores = jnp.einsum("qd,kd->qk", query_rows, key_part, preferred_element_type=jnp.float32)
        key_pos = jnp.arange(key_part.shape[0], dtype=jnp.int32)
        allowed = key_pos[None, :] <= row_pos[:, None]
        probs = jnp.where(
            allowed, jnp.exp(jnp.where(allowed, scores, -1e30) - log_total[:, None]), 0.0
        )
        grad_probs = jnp.einsum(
            "qd,kd->qk", grad_flat, value_part, preferred_element_type=jnp.float32
        )
        grad_scores = (probs * (grad_probs - row_delta[:, None])).astype(jnp.bfloat16)
        return jnp.dot(grad_scores, key_part, preferred_element_type=jnp.float32)

    return query_advance


def key_grad_fold(key_rows, value_rows, key_pos, log_all, delta_all, heads_count):

    def key_advance(carry, piece, start):
        query_part, attn_grad_part = piece
        count = query_part.shape[0]
        scores = jnp.einsum("qd,kd->qk", query_part, key_rows, preferred_element_type=jnp.float32)
        query_pos = jnp.arange(count, dtype=jnp.int32) // heads_count
        allowed = key_pos[None, :] <= query_pos[:, None]
        probs = jnp.where(
            allowed, jnp.exp(jnp.where(allowed, scores, -1e30) - log_all[:, None]), 0.0
        )
        grad_values = jnp.einsum(
            "qk,qd->kd",
            probs.astype(jnp.bfloat16),
            attn_grad_part,
            preferred_element_type=jnp.float32,
        )
        grad_probs = jnp.einsum(
            "qd,kd->qk", attn_grad_part, value_rows, preferred_element_type=jnp.float32
        )
        grad_scores = (probs * (grad_probs - delta_all[:, None])).astype(jnp.bfloat16)
        grad_keys = jnp.einsum(
            "qk,qd->kd", grad_scores, query_part, preferred_element_type=jnp.float32
        )
        return (grad_keys, grad_values)

    return key_advance


def local(hidden_in, norm_gain, qkv_weight, attn_cotangent):
    rows_in = hidden_in[0]
    grad_attn = attn_cotangent[0]
    tokens_here = rows_in.shape[0]
    width = rows_in.shape[1]
    head_size = HD
    heads_count = HEADS
    qcols = heads_count * head_size
    scale = head_size ** (-0.5)
    weight_group, gain_group = (
        lax.all_gather(qkv_weight, "intra", axis=0, tiled=True),
        lax.all_gather(norm_gain, "intra", axis=0, tiled=True),
    )
    weight_full, gain_full = (
        lax.all_gather(weight_group, "inter", axis=0, tiled=True),
        lax.all_gather(gain_group, "inter", axis=0, tiled=True),
    )
    query_pos = lax.axis_index("intra") * tokens_here + jnp.arange(tokens_here, dtype=jnp.int32)
    row_pos = jnp.broadcast_to(query_pos[:, None], (tokens_here, heads_count)).reshape(
        tokens_here * heads_count
    )
    cosine, sine = rope_tables(query_pos, head_size)
    wide_rows = rows_in.astype(jnp.float32)
    inv_rms = lax.rsqrt(jnp.mean(wide_rows * wide_rows, axis=1, keepdims=True) + eps_norm)
    normed = (wide_rows * inv_rms * gain_full.astype(jnp.float32)[None, :]).astype(jnp.bfloat16)
    mixed = jnp.dot(normed, weight_full, preferred_element_type=jnp.float32)
    query_rows = (
        (
            rotate(
                mixed[:, :qcols].reshape(tokens_here, heads_count, head_size),
                cosine[:, None, :],
                sine[:, None, :],
            )
            * scale
        )
        .astype(jnp.bfloat16)
        .reshape(tokens_here * heads_count, head_size)
    )
    key_rows = rotate(mixed[:, qcols : qcols + head_size], cosine, sine).astype(jnp.bfloat16)
    value_rows = mixed[:, qcols + head_size :].astype(jnp.bfloat16)
    grad_flat = grad_attn.reshape(tokens_here * heads_count, head_size)
    flat_rows = tokens_here * heads_count
    forward_step = forward_fold(query_rows, row_pos)
    start_carry = (
        jnp.full((flat_rows,), -1e30, jnp.float32),
        jnp.zeros((flat_rows,), jnp.float32),
        jnp.zeros((flat_rows, head_size), jnp.float32),
    )
    row_top, row_total, weighted = forward_step(
        start_carry,
        (
            lax.all_gather(key_rows, "intra", axis=0, tiled=True),
            lax.all_gather(value_rows, "intra", axis=0, tiled=True),
        ),
        jnp.int32(0),
    )
    attn_flat = (weighted / row_total[:, None]).astype(jnp.bfloat16)
    log_total = row_top + jnp.log(row_total)
    row_delta = jnp.sum(grad_flat.astype(jnp.float32) * attn_flat.astype(jnp.float32), axis=1)
    query_step = query_grad_fold(query_rows, row_pos, grad_flat, log_total, row_delta)
    grad_query = query_step(
        jnp.zeros((flat_rows, head_size), jnp.float32),
        (
            lax.all_gather(key_rows, "intra", axis=0, tiled=True),
            lax.all_gather(value_rows, "intra", axis=0, tiled=True),
        ),
        jnp.int32(0),
    )
    log_all, delta_all = (
        lax.all_gather(log_total, "intra", axis=0, tiled=True),
        lax.all_gather(row_delta, "intra", axis=0, tiled=True),
    )
    key_step = key_grad_fold(key_rows, value_rows, query_pos, log_all, delta_all, heads_count)
    grad_keys, grad_values = key_step(
        (
            jnp.zeros((tokens_here, head_size), jnp.float32),
            jnp.zeros((tokens_here, head_size), jnp.float32),
        ),
        (
            lax.all_gather(query_rows, "intra", axis=0, tiled=True),
            lax.all_gather(grad_flat, "intra", axis=0, tiled=True),
        ),
        jnp.int32(0),
    )
    query_back = (
        unrotate(
            grad_query.reshape(tokens_here, heads_count, head_size),
            cosine[:, None, :],
            sine[:, None, :],
        )
        * scale
    ).reshape(tokens_here, qcols)
    grad_mixed = jnp.concatenate(
        [query_back, unrotate(grad_keys, cosine, sine), grad_values], axis=1
    ).astype(jnp.bfloat16)
    weight_back, gain_back = (weight_full, gain_full)
    gain_wide = gain_back.astype(jnp.float32)[None, :]
    grad_normed = jnp.einsum(
        "tc,dc->td", grad_mixed, weight_back, preferred_element_type=jnp.float32
    )
    inner = jnp.sum(grad_normed * gain_wide * wide_rows, axis=1, keepdims=True)
    grad_rows = (
        gain_wide * grad_normed * inv_rms - wide_rows * inv_rms**3 / width * inner
    ).astype(jnp.bfloat16)
    gain_term = jnp.sum(grad_normed * wide_rows * inv_rms, axis=0)
    normed_cols = lax.all_to_all(normed, "intra", split_axis=1, concat_axis=0, tiled=True)
    group_term = lax.dot_general(
        normed_cols,
        lax.all_gather(grad_mixed, "intra", axis=0, tiled=True),
        (((0,), (0,)), ((), ())),
        preferred_element_type=jnp.float32,
    )
    term_low = lax.optimization_barrier(group_term.astype(jnp.bfloat16))
    gain_sums = lax.psum_scatter(gain_term, "intra", scatter_dimension=0, tiled=True)
    weight_grad, gain_grad = (
        lax.psum_scatter(term_low.astype(jnp.float32), "inter", scatter_dimension=0, tiled=True),
        lax.psum_scatter(gain_sums, "inter", scatter_dimension=0, tiled=True),
    )
    return (attn_flat.reshape(tokens_here, qcols)[None], grad_rows[None], weight_grad, gain_grad)

MESH = pl.DeviceIdType.MESH
CORES = 2
SIDE = 2
GAIN_ROWS = 16


def nt_dot(a, b):
    return lax.dot_general(a, b, (((1,), (1,)), ((), ())), preferred_element_type=jnp.float32)


def tn_dot(a, b):
    return lax.dot_general(a, b, (((0,), (0,)), ((), ())), preferred_element_type=jnp.float32)


def nn_dot(a, b):
    return jnp.dot(a, b, preferred_element_type=jnp.float32)


def fused_kernel(
    n_inter,
    hid_ref, gain_ref, w_ref, ct_ref, cos_ref, sin_ref,
    attn_ref, gin_ref, wg_ref, gg_ref,
    wbuf, nrm, nbuf, kvbuf, gkv, gkv_in, gmbuf, tbuf, rs1, ybuf, rs2, zbuf, rs3, mix,
    ag_send, ag_recv, ex_send, ex_recv, c_send, c_recv, y_send, y_recv, z_send, z_recv,
):
    i = lax.axis_index("inter")
    x = lax.axis_index("intra")
    nz = n_inter // (CORES * SIDE)
    c = lax.rem(i, CORES)
    y = lax.rem(i // CORES, SIDE)
    z = i // (CORES * SIDE)
    toks, width = hid_ref.shape
    rows, cols = w_ref.shape
    half = width // 2
    qcols = HEADS * HD
    scale = HD ** (-0.5)

    def dev(zz, yy, cc, xx):
        return ((zz * SIDE + yy) * CORES + cc, xx)

    def slot(zz, yy, cc, xx):
        return ((zz * SIDE + yy) * CORES + cc) * 2 + xx

    x_peer = dev(z, y, c, 1 - x)
    y_peer = dev(z, 1 - y, c, x)
    c_peer = dev(z, y, 1 - c, x)

    def z_peer(zz):
        return dev(zz, y, c, x)

    own = slot(z, y, c, x)
    wbuf[own, :rows, :] = w_ref[...]
    wbuf[own, rows:, :HD] = jnp.broadcast_to(gain_ref[...], (GAIN_ROWS, HD))
    wbuf[own, rows:, HD:] = jnp.zeros((GAIN_ROWS, cols - HD), jnp.bfloat16)

    barrier = pltpu.get_barrier_semaphore()
    peers = [x_peer, y_peer, c_peer] + [z_peer(lax.rem(z + d, nz)) for d in range(1, nz)]
    for peer in peers:
        pl.semaphore_signal(barrier, inc=1, device_id=peer, device_id_type=MESH)
    pl.semaphore_wait(barrier, len(peers))

    targets = {
        0: x_peer,
        1: y_peer,
        2: z_peer(jnp.minimum(z + 1, nz - 1)),
        3: z_peer(jnp.maximum(z - 1, 0)),
        4: c_peer,
    }
    sent = []

    def ag(link, g):
        return pltpu.make_async_remote_copy(
            src_ref=wbuf.at[g], dst_ref=wbuf.at[g],
            send_sem=ag_send.at[link, g], recv_sem=ag_recv.at[g],
            device_id=targets[link], device_id_type=MESH,
        )

    def send(link, g, cond=None):
        sent.append((link, g, cond))
        if cond is None:
            ag(link, g).start()
        else:
            pl.when(cond)(lambda: ag(link, g).start())

    def arrive(g, cond=None):
        if cond is None:
            ag(0, g).wait_recv()
        else:
            pl.when(cond)(lambda: ag(0, g).wait_recv())

    def both(a, b):
        return b if a is None else jnp.logical_and(a, b)

    up, down = z < nz - 1, z > 0
    send(0, own)
    send(1, own)
    send(2, own, up)
    send(3, own, down)
    send(4, own)
    wide = hid_ref[...].astype(jnp.float32)
    inv = lax.rsqrt(jnp.mean(wide * wide, axis=1, keepdims=True) + eps_norm)
    for d in range(nz):
        sides = [(z, None, None)] if d == 0 else [(z - d, z - d >= 0, 2), (z + d, z + d < nz, 3)]
        if d > 0:
            for zz, ok, link in sides:
                g = slot(zz, y, c, x)
                arrive(g, ok)
                send(link, g, both(ok, up if link == 2 else down))
                send(0, g, ok)
                send(1, g, ok)
                send(4, g, ok)
        for zz, ok, link in sides:
            odd = lax.rem(zz + 2 * nz, 2) == 1
            g = slot(zz, y, c, 1 - x)
            arrive(g, ok)
            send(1, g, both(ok, odd))
            send(4, g, ok)
            g = slot(zz, 1 - y, c, x)
            arrive(g, ok)
            send(0, g, both(ok, jnp.logical_not(odd)))
            send(4, g, ok)
    for zz in range(nz):
        g = slot(zz, 1 - y, c, 1 - x)
        arrive(g)
        send(4, g)
    for zz in range(nz):
        for yy in range(SIDE):
            for xx in range(2):
                arrive(slot(zz, yy, 1 - c, xx))

    acc = jnp.zeros((toks, cols), jnp.float32)
    for p in range(n_inter):
        parts = []
        for q in range(2):
            g = 2 * p + q
            lanes = slice(g * rows, (g + 1) * rows)
            gain = wbuf[g, rows : rows + 1, :rows].astype(jnp.float32)
            part = (hid_ref[:, lanes].astype(jnp.float32) * inv * gain).astype(jnp.bfloat16)
            nrm[:, lanes] = part
            parts.append(part)
        acc = acc + nn_dot(
            jnp.concatenate(parts, axis=1),
            jnp.concatenate([wbuf[2 * p, :rows, :], wbuf[2 * p + 1, :rows, :]], axis=0),
        )
    mix[...] = acc

    cosine = cos_ref[pl.ds(pl.multiple_of(x * toks, toks), toks), :]
    sine = sin_ref[pl.ds(pl.multiple_of(x * toks, toks), toks), :]

    def rope(u):
        return u * cosine + pltpu.roll(u, HD // 2, 1) * sine

    def unrope(u):
        return u * cosine - pltpu.roll(u, HD // 2, 1) * sine

    here = pl.ds(pl.multiple_of(x * toks, toks), toks)
    there = pl.ds(pl.multiple_of((1 - x) * toks, toks), toks)

    def exchange(k, src, dst):
        return pltpu.make_async_remote_copy(
            src_ref=src, dst_ref=dst, send_sem=ex_send.at[k], recv_sem=ex_recv.at[k],
            device_id=x_peer, device_id_type=MESH,
        )

    kvbuf[here, :HD] = rope(acc[:, qcols : qcols + HD]).astype(jnp.bfloat16)
    kvbuf[here, HD:] = acc[:, qcols + HD :].astype(jnp.bfloat16)
    query = [(rope(acc[:, h * HD : (h + 1) * HD]) * scale).astype(jnp.bfloat16) for h in range(HEADS)]
    query = jnp.concatenate(query, axis=0)
    kv_copy = exchange(0, kvbuf.at[here], kvbuf.at[here])
    kv_copy.start()
    keep = pl.ds(pl.multiple_of(x * half, half), half)
    give = pl.ds(pl.multiple_of((1 - x) * half, half), half)
    norm_copy = exchange(1, nrm.at[:, give], nbuf.at[here])
    norm_copy.start()
    nbuf[here, :] = nrm[:, keep]
    kv_copy.wait()

    flat = HEADS * toks
    keys, values = kvbuf[:, :HD], kvbuf[:, HD:]
    row_pos = x * toks + lax.rem(lax.broadcasted_iota(jnp.int32, (flat, 2 * toks), 0), toks)
    allowed = lax.broadcasted_iota(jnp.int32, (flat, 2 * toks), 1) <= row_pos
    scores = jnp.where(allowed, nt_dot(query, keys), -1e30)
    top = jnp.max(scores, axis=1, keepdims=True)
    numbers = jnp.where(allowed, jnp.exp(scores - top), 0.0)
    total = jnp.sum(numbers, axis=1, keepdims=True)
    high = numbers.astype(jnp.bfloat16)
    low = (numbers - high.astype(jnp.float32)).astype(jnp.bfloat16)
    attn = ((nn_dot(high, values) + nn_dot(low, values)) / total).astype(jnp.bfloat16)
    for h in range(HEADS):
        attn_ref[:, h * HD : (h + 1) * HD] = attn[h * toks : (h + 1) * toks]
    grad = jnp.concatenate([ct_ref[:, h * HD : (h + 1) * HD] for h in range(HEADS)], axis=0)
    delta = jnp.sum(grad.astype(jnp.float32) * attn.astype(jnp.float32), axis=1, keepdims=True)
    probs = numbers / total
    grad_scores = (probs * (nt_dot(grad, values) - delta)).astype(jnp.bfloat16)
    gkv[:, :HD] = tn_dot(grad_scores, query)
    gkv[:, HD:] = tn_dot(probs.astype(jnp.bfloat16), grad)
    gkv_copy = exchange(2, gkv.at[there], gkv_in)
    gkv_copy.start()
    grad_query = nn_dot(grad_scores, keys)
    for h in range(HEADS):
        gmbuf[here, h * HD : (h + 1) * HD] = (
            unrope(grad_query[h * toks : (h + 1) * toks]) * scale
        ).astype(jnp.bfloat16)
    gkv_copy.wait()
    own_kv = gkv[here, :] + gkv_in[...]
    gmbuf[here, qcols : qcols + HD] = unrope(own_kv[:, :HD]).astype(jnp.bfloat16)
    gmbuf[here, qcols + HD :] = own_kv[:, HD:].astype(jnp.bfloat16)
    gm_copy = exchange(3, gmbuf.at[here], gmbuf.at[here])
    gm_copy.start()

    gm = gmbuf[here, :]
    inner = jnp.sum(gm.astype(jnp.float32) * mix[...], axis=1, keepdims=True)
    back = inner * (inv * inv / width)

    def grad_rows(first, last):
        for g in range(first, last):
            lanes = slice(g * rows, (g + 1) * rows)
            gain = wbuf[g, rows : rows + 1, :rows].astype(jnp.float32)
            part = nt_dot(gm, wbuf[g, :rows, :])
            gin_ref[:, lanes] = (
                gain * part * inv - hid_ref[:, lanes].astype(jnp.float32) * back
            ).astype(jnp.bfloat16)

    pieces = nz + 1
    marks = [2 * n_inter * k // pieces for k in range(pieces + 1)]
    grad_rows(marks[0], marks[1])
    norm_copy.wait()
    gm_copy.wait()

    both_gm = gmbuf[...]

    def term(k, cc):
        j = k * CORES + cc
        lanes = pl.ds(pl.multiple_of(j * rows, rows), rows)
        tbuf[j] = tn_dot(nbuf[:, lanes], both_gm).astype(jnp.bfloat16)

    def to_core(k):
        return pltpu.make_async_remote_copy(
            src_ref=tbuf.at[k * CORES + 1 - c], dst_ref=rs1.at[k],
            send_sem=c_send.at[k], recv_sem=c_recv.at[k], device_id=c_peer, device_id_type=MESH,
        )

    def to_y(zz):
        return pltpu.make_async_remote_copy(
            src_ref=ybuf.at[zz], dst_ref=rs2.at[zz],
            send_sem=y_send.at[zz], recv_sem=y_recv.at[zz], device_id=y_peer, device_id_type=MESH,
        )

    def to_z(d):
        return pltpu.make_async_remote_copy(
            src_ref=zbuf.at[d - 1], dst_ref=rs3.at[d - 1],
            send_sem=z_send.at[d - 1], recv_sem=z_recv.at[d - 1],
            device_id=z_peer(lax.rem(z + d, nz)), device_id_type=MESH,
        )

    order = [(d, lax.rem(z + d, nz)) for d in list(range(1, nz)) + [0]]

    def core_sum(k):
        to_core(k).wait_recv()
        return tbuf[k * CORES + c].astype(jnp.float32) + rs1[k].astype(jnp.float32)

    for yy in (1 - y, y):
        for d, zz in order:
            term(zz * SIDE + yy, 1 - c)
            to_core(zz * SIDE + yy).start()
            term(zz * SIDE + yy, c)
            if yy is not y:
                pass
        if yy is not y:
            for d, zz in order:
                ybuf[zz] = core_sum(zz * SIDE + yy).astype(jnp.bfloat16)
                to_y(zz).start()
    kept = None
    for n, (d, zz) in enumerate(order):
        grad_rows(marks[n + 1], marks[n + 2])
        part = core_sum(zz * SIDE + y)
        to_y(zz).wait_recv()
        part = part + rs2[zz].astype(jnp.float32)
        if d:
            zbuf[d - 1] = part.astype(jnp.bfloat16)
            to_z(d).start()
        else:
            wg_ref[...] = part
    result = wg_ref[...]
    for d in range(1, nz):
        to_z(d).wait_recv()
        result = result + rs3[d - 1].astype(jnp.float32)
    wg_ref[...] = result
    block = x * n_inter + i
    mixed_sum = wbuf[block, :rows, :].astype(jnp.float32) * result
    lanes_sum = mixed_sum[:, :HD]
    for k in range(1, cols // HD):
        lanes_sum = lanes_sum + mixed_sum[:, k * HD : (k + 1) * HD]
    gain = wbuf[block, rows : rows + 1, :rows].astype(jnp.float32)
    gg_ref[...] = jnp.sum(lanes_sum.T, axis=0, keepdims=True) / gain

    for link, g, cond in sent:
        if cond is None:
            ag(link, g).wait_send()
        else:
            pl.when(cond)(functools.partial(lambda l, s: ag(l, s).wait_send(), link, g))
    for k in range(nz * SIDE):
        to_core(k).wait_send()
    for zz in range(nz):
        to_y(zz).wait_send()
    for d in range(1, nz):
        to_z(d).wait_send()


def fused(n_inter, hidden_in, norm_gain, qkv_weight, attn_cotangent):
    toks, width = hidden_in.shape[1:]
    rows, cols = qkv_weight.shape
    nz = n_inter // (CORES * SIDE)
    chips = nz * SIDE
    freqs = rope_base ** (-np.arange(HD // 2, dtype=np.float32) / np.float32(HD // 2))
    angles = (np.arange(2 * toks, dtype=np.float32)[:, None] * freqs.astype(np.float32)[None, :]).astype(np.float32)
    cosine = np.concatenate([np.cos(angles)] * 2, axis=1).astype(np.float32)
    sine = np.concatenate([-np.sin(angles), np.sin(angles)], axis=1).astype(np.float32)
    bf, f32, dma = jnp.bfloat16, jnp.float32, pltpu.SemaphoreType.DMA
    vmem = pl.BlockSpec(memory_space=pltpu.VMEM)
    attn, gin, wg, gg = pl.pallas_call(
        functools.partial(fused_kernel, n_inter),
        out_shape=(
            jax.ShapeDtypeStruct((toks, HEADS * HD), bf),
            jax.ShapeDtypeStruct((toks, width), bf),
            jax.ShapeDtypeStruct((rows, cols), f32),
            jax.ShapeDtypeStruct((1, rows), f32),
        ),
        in_specs=[vmem] * 6,
        out_specs=(vmem,) * 4,
        scratch_shapes=[
            pltpu.VMEM((2 * n_inter, rows + GAIN_ROWS, cols), bf),
            pltpu.VMEM((toks, width), bf),
            pltpu.VMEM((2 * toks, width // 2), bf),
            pltpu.VMEM((2 * toks, 2 * HD), bf),
            pltpu.VMEM((2 * toks, 2 * HD), f32),
            pltpu.VMEM((toks, 2 * HD), f32),
            pltpu.VMEM((2 * toks, cols), bf),
            pltpu.VMEM((n_inter, rows, cols), bf),
            pltpu.VMEM((chips, rows, cols), bf),
            pltpu.VMEM((nz, rows, cols), bf),
            pltpu.VMEM((nz, rows, cols), bf),
            pltpu.VMEM((max(nz - 1, 1), rows, cols), bf),
            pltpu.VMEM((max(nz - 1, 1), rows, cols), bf),
            pltpu.VMEM((toks, cols), f32),
            dma((5, 2 * n_inter)), dma((2 * n_inter,)),
            dma((4,)), dma((4,)),
            dma((chips,)), dma((chips,)),
            dma((nz,)), dma((nz,)),
            dma((max(nz - 1, 1),)), dma((max(nz - 1, 1),)),
        ],
        compiler_params=pltpu.CompilerParams(
            collective_id=0, has_side_effects=True, vmem_limit_bytes=60 * 2**20
        ),
    )(hidden_in[0], norm_gain[None], qkv_weight, attn_cotangent[0], cosine, sine)
    return attn[None], gin[None], wg, gg[0]


def solution(mesh):
    n_inter, n_intra = mesh.shape["inter"], mesh.shape["intra"]

    def body(hidden_in, norm_gain, qkv_weight, attn_cotangent):
        fits = n_intra == 2 and n_inter % (CORES * SIDE) == 0
        fits = fits and qkv_weight.shape[0] == HD and hidden_in.shape[0] == 1
        fits = fits and hidden_in.shape[1] % HD == 0
        if fits:
            return fused(n_inter, hidden_in, norm_gain, qkv_weight, attn_cotangent)
        return local(hidden_in, norm_gain, qkv_weight, attn_cotangent)

    return jax.shard_map(
        body,
        mesh=mesh,
        in_specs=(
            P("inter", "intra", None),
            P(("inter", "intra")),
            P(("inter", "intra"), None),
            P("inter", "intra", None),
        ),
        out_specs=(
            P("inter", "intra", None),
            P("inter", "intra", None),
            P(("intra", "inter"), None),
            P(("intra", "inter")),
        ),
        check_vma=False,
    )
```

```python
import functools
import jax
import jax.numpy as jnp
import numpy as np
from jax import lax
from jax.experimental import pallas as pl
from jax.experimental.pallas import tpu as pltpu
from jax.sharding import PartitionSpec as P

HD = 128
HEADS = 4


eps_norm = 1e-05
rope_base = 500000.0


def rope_tables(positions, head_size):
    half_size = head_size // 2
    freqs = rope_base ** (-jnp.arange(half_size, dtype=jnp.float32) / half_size)
    angles = positions.astype(jnp.float32)[:, None] * freqs[None, :]
    return (jnp.cos(angles), jnp.sin(angles))


def rotate(values_in, cosine, sine):
    half_size = values_in.shape[-1] // 2
    first, second = (values_in[..., :half_size], values_in[..., half_size:])
    return jnp.concatenate(
        [first * cosine - second * sine, second * cosine + first * sine], axis=-1
    )


def unrotate(grad_out, cosine, sine):
    half_size = grad_out.shape[-1] // 2
    first, second = (grad_out[..., :half_size], grad_out[..., half_size:])
    return jnp.concatenate(
        [first * cosine + second * sine, second * cosine - first * sine], axis=-1
    )


def forward_fold(query_rows, row_pos):

    def forward_advance(carry, piece, start):
        row_top, row_total, weighted = carry
        key_part, value_part = piece
        scores = jnp.einsum("qd,kd->qk", query_rows, key_part, preferred_element_type=jnp.float32)
        key_pos = jnp.arange(key_part.shape[0], dtype=jnp.int32)
        allowed = key_pos[None, :] <= row_pos[:, None]
        scores = jnp.where(allowed, scores, -1e30)
        new_top = jnp.maximum(row_top, jnp.max(scores, axis=1))
        numbers = jnp.where(allowed, jnp.exp(scores - new_top[:, None]), 0.0)
        row_total = jnp.sum(numbers, axis=1)
        weighted = jnp.dot(
            numbers,
            value_part.astype(jnp.float32),
            precision=lax.Precision.HIGHEST,
            preferred_element_type=jnp.float32,
        )
        return (new_top, row_total, weighted)

    return forward_advance


def query_grad_fold(query_rows, row_pos, grad_flat, log_total, row_delta):

    def query_advance(grad_query, piece, start):
        key_part, value_part = piece
        scores = jnp.einsum("qd,kd->qk", query_rows, key_part, preferred_element_type=jnp.float32)
        key_pos = jnp.arange(key_part.shape[0], dtype=jnp.int32)
        allowed = key_pos[None, :] <= row_pos[:, None]
        probs = jnp.where(
            allowed, jnp.exp(jnp.where(allowed, scores, -1e30) - log_total[:, None]), 0.0
        )
        grad_probs = jnp.einsum(
            "qd,kd->qk", grad_flat, value_part, preferred_element_type=jnp.float32
        )
        grad_scores = (probs * (grad_probs - row_delta[:, None])).astype(jnp.bfloat16)
        return jnp.dot(grad_scores, key_part, preferred_element_type=jnp.float32)

    return query_advance


def key_grad_fold(key_rows, value_rows, key_pos, log_all, delta_all, heads_count):

    def key_advance(carry, piece, start):
        query_part, attn_grad_part = piece
        count = query_part.shape[0]
        scores = jnp.einsum("qd,kd->qk", query_part, key_rows, preferred_element_type=jnp.float32)
        query_pos = jnp.arange(count, dtype=jnp.int32) // heads_count
        allowed = key_pos[None, :] <= query_pos[:, None]
        probs = jnp.where(
            allowed, jnp.exp(jnp.where(allowed, scores, -1e30) - log_all[:, None]), 0.0
        )
        grad_values = jnp.einsum(
            "qk,qd->kd",
            probs.astype(jnp.bfloat16),
            attn_grad_part,
            preferred_element_type=jnp.float32,
        )
        grad_probs = jnp.einsum(
            "qd,kd->qk", attn_grad_part, value_rows, preferred_element_type=jnp.float32
        )
        grad_scores = (probs * (grad_probs - delta_all[:, None])).astype(jnp.bfloat16)
        grad_keys = jnp.einsum(
            "qk,qd->kd", grad_scores, query_part, preferred_element_type=jnp.float32
        )
        return (grad_keys, grad_values)

    return key_advance


def local(hidden_in, norm_gain, qkv_weight, attn_cotangent):
    rows_in = hidden_in[0]
    grad_attn = attn_cotangent[0]
    tokens_here = rows_in.shape[0]
    width = rows_in.shape[1]
    head_size = HD
    heads_count = HEADS
    qcols = heads_count * head_size
    scale = head_size ** (-0.5)
    weight_group, gain_group = (
        lax.all_gather(qkv_weight, "intra", axis=0, tiled=True),
        lax.all_gather(norm_gain, "intra", axis=0, tiled=True),
    )
    weight_full, gain_full = (
        lax.all_gather(weight_group, "inter", axis=0, tiled=True),
        lax.all_gather(gain_group, "inter", axis=0, tiled=True),
    )
    query_pos = lax.axis_index("intra") * tokens_here + jnp.arange(tokens_here, dtype=jnp.int32)
    row_pos = jnp.broadcast_to(query_pos[:, None], (tokens_here, heads_count)).reshape(
        tokens_here * heads_count
    )
    cosine, sine = rope_tables(query_pos, head_size)
    wide_rows = rows_in.astype(jnp.float32)
    inv_rms = lax.rsqrt(jnp.mean(wide_rows * wide_rows, axis=1, keepdims=True) + eps_norm)
    normed = (wide_rows * inv_rms * gain_full.astype(jnp.float32)[None, :]).astype(jnp.bfloat16)
    mixed = jnp.dot(normed, weight_full, preferred_element_type=jnp.float32)
    query_rows = (
        (
            rotate(
                mixed[:, :qcols].reshape(tokens_here, heads_count, head_size),
                cosine[:, None, :],
                sine[:, None, :],
            )
            * scale
        )
        .astype(jnp.bfloat16)
        .reshape(tokens_here * heads_count, head_size)
    )
    key_rows = rotate(mixed[:, qcols : qcols + head_size], cosine, sine).astype(jnp.bfloat16)
    value_rows = mixed[:, qcols + head_size :].astype(jnp.bfloat16)
    grad_flat = grad_attn.reshape(tokens_here * heads_count, head_size)
    flat_rows = tokens_here * heads_count
    forward_step = forward_fold(query_rows, row_pos)
    start_carry = (
        jnp.full((flat_rows,), -1e30, jnp.float32),
        jnp.zeros((flat_rows,), jnp.float32),
        jnp.zeros((flat_rows, head_size), jnp.float32),
    )
    row_top, row_total, weighted = forward_step(
        start_carry,
        (
            lax.all_gather(key_rows, "intra", axis=0, tiled=True),
            lax.all_gather(value_rows, "intra", axis=0, tiled=True),
        ),
        jnp.int32(0),
    )
    attn_flat = (weighted / row_total[:, None]).astype(jnp.bfloat16)
    log_total = row_top + jnp.log(row_total)
    row_delta = jnp.sum(grad_flat.astype(jnp.float32) * attn_flat.astype(jnp.float32), axis=1)
    query_step = query_grad_fold(query_rows, row_pos, grad_flat, log_total, row_delta)
    grad_query = query_step(
        jnp.zeros((flat_rows, head_size), jnp.float32),
        (
            lax.all_gather(key_rows, "intra", axis=0, tiled=True),
            lax.all_gather(value_rows, "intra", axis=0, tiled=True),
        ),
        jnp.int32(0),
    )
    log_all, delta_all = (
        lax.all_gather(log_total, "intra", axis=0, tiled=True),
        lax.all_gather(row_delta, "intra", axis=0, tiled=True),
    )
    key_step = key_grad_fold(key_rows, value_rows, query_pos, log_all, delta_all, heads_count)
    grad_keys, grad_values = key_step(
        (
            jnp.zeros((tokens_here, head_size), jnp.float32),
            jnp.zeros((tokens_here, head_size), jnp.float32),
        ),
        (
            lax.all_gather(query_rows, "intra", axis=0, tiled=True),
            lax.all_gather(grad_flat, "intra", axis=0, tiled=True),
        ),
        jnp.int32(0),
    )
    query_back = (
        unrotate(
            grad_query.reshape(tokens_here, heads_count, head_size),
            cosine[:, None, :],
            sine[:, None, :],
        )
        * scale
    ).reshape(tokens_here, qcols)
    grad_mixed = jnp.concatenate(
        [query_back, unrotate(grad_keys, cosine, sine), grad_values], axis=1
    ).astype(jnp.bfloat16)
    weight_back, gain_back = (weight_full, gain_full)
    gain_wide = gain_back.astype(jnp.float32)[None, :]
    grad_normed = jnp.einsum(
        "tc,dc->td", grad_mixed, weight_back, preferred_element_type=jnp.float32
    )
    inner = jnp.sum(grad_normed * gain_wide * wide_rows, axis=1, keepdims=True)
    grad_rows = (
        gain_wide * grad_normed * inv_rms - wide_rows * inv_rms**3 / width * inner
    ).astype(jnp.bfloat16)
    gain_term = jnp.sum(grad_normed * wide_rows * inv_rms, axis=0)
    normed_cols = lax.all_to_all(normed, "intra", split_axis=1, concat_axis=0, tiled=True)
    group_term = lax.dot_general(
        normed_cols,
        lax.all_gather(grad_mixed, "intra", axis=0, tiled=True),
        (((0,), (0,)), ((), ())),
        preferred_element_type=jnp.float32,
    )
    term_low = lax.optimization_barrier(group_term.astype(jnp.bfloat16))
    gain_sums = lax.psum_scatter(gain_term, "intra", scatter_dimension=0, tiled=True)
    weight_grad, gain_grad = (
        lax.psum_scatter(term_low.astype(jnp.float32), "inter", scatter_dimension=0, tiled=True),
        lax.psum_scatter(gain_sums, "inter", scatter_dimension=0, tiled=True),
    )
    return (attn_flat.reshape(tokens_here, qcols)[None], grad_rows[None], weight_grad, gain_grad)

MESH = pl.DeviceIdType.MESH
CORES = 2
SIDE = 2
GAIN_ROWS = 16


def nt_dot(a, b):
    return lax.dot_general(a, b, (((1,), (1,)), ((), ())), preferred_element_type=jnp.float32)


def tn_dot(a, b):
    return lax.dot_general(a, b, (((0,), (0,)), ((), ())), preferred_element_type=jnp.float32)


def nn_dot(a, b):
    return jnp.dot(a, b, preferred_element_type=jnp.float32)


def fused_kernel(
    n_inter,
    hid_ref, gain_ref, w_ref, ct_ref, cos_ref, sin_ref,
    attn_ref, gin_ref, wg_ref, gg_ref,
    wbuf, nrm, nbuf, kvbuf, gkv, gkv_in, gmbuf, tbuf, rs1, ybuf, rs2, zbuf, rs3, mix,
    ag_send, ag_recv, ex_send, ex_recv, c_send, c_recv, y_send, y_recv, z_send, z_recv,
):
    i = lax.axis_index("inter")
    x = lax.axis_index("intra")
    nz = n_inter // (CORES * SIDE)
    c = lax.rem(i, CORES)
    y = lax.rem(i // CORES, SIDE)
    z = i // (CORES * SIDE)
    toks, width = hid_ref.shape
    rows, cols = w_ref.shape
    half = width // 2
    qcols = HEADS * HD
    scale = HD ** (-0.5)

    def dev(zz, yy, cc, xx):
        return ((zz * SIDE + yy) * CORES + cc, xx)

    def slot(zz, yy, cc, xx):
        return ((zz * SIDE + yy) * CORES + cc) * 2 + xx

    x_peer = dev(z, y, c, 1 - x)
    y_peer = dev(z, 1 - y, c, x)
    c_peer = dev(z, y, 1 - c, x)

    def z_peer(zz):
        return dev(zz, y, c, x)

    own = slot(z, y, c, x)
    wbuf[own, :rows, :] = w_ref[...]
    wbuf[own, rows:, :HD] = jnp.broadcast_to(gain_ref[...], (GAIN_ROWS, HD))
    wbuf[own, rows:, HD:] = jnp.zeros((GAIN_ROWS, cols - HD), jnp.bfloat16)

    barrier = pltpu.get_barrier_semaphore()
    peers = [x_peer, y_peer, c_peer] + [z_peer(lax.rem(z + d, nz)) for d in range(1, nz)]
    for peer in peers:
        pl.semaphore_signal(barrier, inc=1, device_id=peer, device_id_type=MESH)
    pl.semaphore_wait(barrier, len(peers))

    targets = {
        0: x_peer,
        1: y_peer,
        2: z_peer(jnp.minimum(z + 1, nz - 1)),
        3: z_peer(jnp.maximum(z - 1, 0)),
        4: c_peer,
    }
    sent = []

    def ag(link, g):
        return pltpu.make_async_remote_copy(
            src_ref=wbuf.at[g], dst_ref=wbuf.at[g],
            send_sem=ag_send.at[link, g], recv_sem=ag_recv.at[g],
            device_id=targets[link], device_id_type=MESH,
        )

    def send(link, g, cond=None):
        sent.append((link, g, cond))
        if cond is None:
            ag(link, g).start()
        else:
            pl.when(cond)(lambda: ag(link, g).start())

    def arrive(g, cond=None):
        if cond is None:
            ag(0, g).wait_recv()
        else:
            pl.when(cond)(lambda: ag(0, g).wait_recv())

    def both(a, b):
        return b if a is None else jnp.logical_and(a, b)

    up, down = z < nz - 1, z > 0
    send(0, own)
    send(1, own)
    send(2, own, up)
    send(3, own, down)
    send(4, own)
    wide = hid_ref[...].astype(jnp.float32)
    inv = lax.rsqrt(jnp.mean(wide * wide, axis=1, keepdims=True) + eps_norm)
    mix[...] = jnp.zeros((toks, cols), jnp.float32)
    span = lambda g: pl.ds(pl.multiple_of(g * rows, rows), rows)

    def absorb(g):
        gain = wbuf[g, rows : rows + 1, :rows].astype(jnp.float32)
        part = (hid_ref[:, span(g)].astype(jnp.float32) * inv * gain).astype(jnp.bfloat16)
        nrm[:, span(g)] = part
        mix[...] += nn_dot(part, wbuf[g, :rows, :])

    def absorb_when(g, cond):
        if cond is None:
            absorb(g)
        else:
            pl.when(cond)(lambda: absorb(g))

    def sides(d):
        if d == 0:
            return [(z, None, None)]
        return [(z - d, z - d >= 0, 2), (z + d, z + d < nz, 3)]

    def onward(link):
        return up if link == 2 else down

    late = []

    def done(zz, yy, xx, ok):
        late.append((zz, yy, xx, ok))
        absorb_when(slot(zz, yy, c, xx), ok)

    def drain(count):
        for _ in range(min(count, len(late))):
            zz, yy, xx, ok = late.pop(0)
            g = slot(zz, yy, 1 - c, xx)
            arrive(g, ok)
            absorb_when(g, ok)

    def column(d):
        for zz, ok, link in sides(d):
            g = slot(zz, y, c, x)
            arrive(g, ok)
            send(link, g, both(ok, onward(link)))
            for k in (0, 1, 4):
                send(k, g, ok)
        for zz, ok, link in sides(d):
            done(zz, y, x, ok)

    direct = [d for d in range(nz) if d == 0 or d >= 3]

    def side(d):
        for zz, ok, link in sides(d):
            odd = lax.rem(zz + 2 * nz, 2) == 1
            g = slot(zz, y, c, 1 - x)
            arrive(g, ok)
            if d in direct:
                send(1, g, both(ok, odd))
            send(4, g, ok)
            g = slot(zz, 1 - y, c, x)
            arrive(g, ok)
            if d in direct:
                send(0, g, both(ok, jnp.logical_not(odd)))
            send(4, g, ok)
        for zz, ok, link in sides(d):
            done(zz, y, 1 - x, ok)
            done(zz, 1 - y, x, ok)

    def diagonal(d):
        for zz, ok, link in sides(d):
            g = slot(zz, 1 - y, c, 1 - x)
            arrive(g, ok)
            if d + 1 < nz and d + 1 not in direct:
                if d == 0:
                    send(2, g, up)
                    send(3, g, down)
                else:
                    send(link, g, both(ok, onward(link)))
            send(4, g, ok)
        for zz, ok, link in sides(d):
            done(zz, 1 - y, 1 - x, ok)

    done(z, y, x, None)
    steps = [(d * 3, column, d) for d in range(1, nz)]
    steps += [(d * 3 + 4, side, d) for d in range(nz)]
    steps += [(d * 3 + 8, diagonal, d) for d in range(nz)]
    for _, step, d in sorted(steps, key=lambda e: e[0]):
        waiting = len(late)
        step(d)
        drain(waiting)
    drain(len(late))
    acc = mix[...]

    cosine = cos_ref[pl.ds(pl.multiple_of(x * toks, toks), toks), :]
    sine = sin_ref[pl.ds(pl.multiple_of(x * toks, toks), toks), :]

    def rope(u):
        return u * cosine + pltpu.roll(u, HD // 2, 1) * sine

    def unrope(u):
        return u * cosine - pltpu.roll(u, HD // 2, 1) * sine

    here = pl.ds(pl.multiple_of(x * toks, toks), toks)
    there = pl.ds(pl.multiple_of((1 - x) * toks, toks), toks)

    def exchange(k, src, dst):
        return pltpu.make_async_remote_copy(
            src_ref=src, dst_ref=dst, send_sem=ex_send.at[k], recv_sem=ex_recv.at[k],
            device_id=x_peer, device_id_type=MESH,
        )

    kvbuf[here, :HD] = rope(acc[:, qcols : qcols + HD]).astype(jnp.bfloat16)
    kvbuf[here, HD:] = acc[:, qcols + HD :].astype(jnp.bfloat16)
    query = [(rope(acc[:, h * HD : (h + 1) * HD]) * scale).astype(jnp.bfloat16) for h in range(HEADS)]
    query = jnp.concatenate(query, axis=0)
    kv_copy = exchange(0, kvbuf.at[here], kvbuf.at[here])
    kv_copy.start()
    keep = pl.ds(pl.multiple_of(x * half, half), half)
    give = pl.ds(pl.multiple_of((1 - x) * half, half), half)
    norm_copy = exchange(1, nrm.at[:, give], nbuf.at[here])
    norm_copy.start()
    nbuf[here, :] = nrm[:, keep]
    kv_copy.wait()

    flat = HEADS * toks
    keys, values = kvbuf[:, :HD], kvbuf[:, HD:]
    row_pos = x * toks + lax.rem(lax.broadcasted_iota(jnp.int32, (flat, 2 * toks), 0), toks)
    allowed = lax.broadcasted_iota(jnp.int32, (flat, 2 * toks), 1) <= row_pos
    scores = jnp.where(allowed, nt_dot(query, keys), -1e30)
    top = jnp.max(scores, axis=1, keepdims=True)
    numbers = jnp.where(allowed, jnp.exp(scores - top), 0.0)
    total = jnp.sum(numbers, axis=1, keepdims=True)
    high = numbers.astype(jnp.bfloat16)
    low = (numbers - high.astype(jnp.float32)).astype(jnp.bfloat16)
    attn = ((nn_dot(high, values) + nn_dot(low, values)) / total).astype(jnp.bfloat16)
    for h in range(HEADS):
        attn_ref[:, h * HD : (h + 1) * HD] = attn[h * toks : (h + 1) * toks]
    grad = jnp.concatenate([ct_ref[:, h * HD : (h + 1) * HD] for h in range(HEADS)], axis=0)
    delta = jnp.sum(grad.astype(jnp.float32) * attn.astype(jnp.float32), axis=1, keepdims=True)
    probs = numbers / total
    grad_scores = (probs * (nt_dot(grad, values) - delta)).astype(jnp.bfloat16)
    gkv[:, :HD] = tn_dot(grad_scores, query)
    gkv[:, HD:] = tn_dot(probs.astype(jnp.bfloat16), grad)
    gkv_copy = exchange(2, gkv.at[there], gkv_in)
    gkv_copy.start()
    grad_query = nn_dot(grad_scores, keys)
    for h in range(HEADS):
        gmbuf[here, h * HD : (h + 1) * HD] = (
            unrope(grad_query[h * toks : (h + 1) * toks]) * scale
        ).astype(jnp.bfloat16)
    gkv_copy.wait()
    own_kv = gkv[here, :] + gkv_in[...]
    gmbuf[here, qcols : qcols + HD] = unrope(own_kv[:, :HD]).astype(jnp.bfloat16)
    gmbuf[here, qcols + HD :] = own_kv[:, HD:].astype(jnp.bfloat16)
    gm_copy = exchange(3, gmbuf.at[here], gmbuf.at[here])
    gm_copy.start()

    gm = gmbuf[here, :]
    inner = jnp.sum(gm.astype(jnp.float32) * mix[...], axis=1, keepdims=True)
    back = inner * (inv * inv / width)

    def grad_rows(first, last):
        for g in range(first, last):
            lanes = slice(g * rows, (g + 1) * rows)
            gain = wbuf[g, rows : rows + 1, :rows].astype(jnp.float32)
            part = nt_dot(gm, wbuf[g, :rows, :])
            gin_ref[:, lanes] = (
                gain * part * inv - hid_ref[:, lanes].astype(jnp.float32) * back
            ).astype(jnp.bfloat16)

    pieces = nz + 1
    marks = [2 * n_inter * k // pieces for k in range(pieces + 1)]
    grad_rows(marks[0], marks[1])
    norm_copy.wait()
    gm_copy.wait()

    both_gm = gmbuf[...]

    def term(k, cc):
        j = k * CORES + cc
        lanes = pl.ds(pl.multiple_of(j * rows, rows), rows)
        tbuf[j] = tn_dot(nbuf[:, lanes], both_gm).astype(jnp.bfloat16)

    def to_core(k):
        return pltpu.make_async_remote_copy(
            src_ref=tbuf.at[k * CORES + 1 - c], dst_ref=rs1.at[k],
            send_sem=c_send.at[k], recv_sem=c_recv.at[k], device_id=c_peer, device_id_type=MESH,
        )

    def to_y(zz):
        return pltpu.make_async_remote_copy(
            src_ref=ybuf.at[zz], dst_ref=rs2.at[zz],
            send_sem=y_send.at[zz], recv_sem=y_recv.at[zz], device_id=y_peer, device_id_type=MESH,
        )

    def to_z(d):
        return pltpu.make_async_remote_copy(
            src_ref=zbuf.at[d - 1], dst_ref=rs3.at[d - 1],
            send_sem=z_send.at[d - 1], recv_sem=z_recv.at[d - 1],
            device_id=z_peer(lax.rem(z + d, nz)), device_id_type=MESH,
        )

    order = [(d, lax.rem(z + d, nz)) for d in list(range(1, nz)) + [0]]

    def core_sum(k):
        to_core(k).wait_recv()
        return tbuf[k * CORES + c].astype(jnp.float32) + rs1[k].astype(jnp.float32)

    def to_y_side(zz):
        ybuf[zz] = core_sum(zz * SIDE + 1 - y).astype(jnp.bfloat16)
        to_y(zz).start()

    last = None
    for d, zz in order:
        k = zz * SIDE + 1 - y
        term(k, 1 - c)
        to_core(k).start()
        term(k, c)
        if last is not None:
            to_y_side(last)
        last = zz
    for n, (d, zz) in enumerate(order):
        k = zz * SIDE + y
        term(k, 1 - c)
        to_core(k).start()
        if n == 0:
            to_y_side(last)
        term(k, c)
    for n, (d, zz) in enumerate(order):
        grad_rows(marks[n + 1], marks[n + 2])
        part = core_sum(zz * SIDE + y)
        to_y(zz).wait_recv()
        part = part + rs2[zz].astype(jnp.float32)
        if d:
            zbuf[d - 1] = part.astype(jnp.bfloat16)
            to_z(d).start()
        else:
            wg_ref[...] = part
    result = wg_ref[...]
    for d in range(1, nz):
        to_z(d).wait_recv()
        result = result + rs3[d - 1].astype(jnp.float32)
    wg_ref[...] = result
    block = x * n_inter + i
    mixed_sum = wbuf[block, :rows, :].astype(jnp.float32) * result
    lanes_sum = mixed_sum[:, :HD]
    for k in range(1, cols // HD):
        lanes_sum = lanes_sum + mixed_sum[:, k * HD : (k + 1) * HD]
    gain = wbuf[block, rows : rows + 1, :rows].astype(jnp.float32)
    gg_ref[...] = jnp.sum(lanes_sum.T, axis=0, keepdims=True) / gain

    for link, g, cond in sent:
        if cond is None:
            ag(link, g).wait_send()
        else:
            pl.when(cond)(functools.partial(lambda l, s: ag(l, s).wait_send(), link, g))
    for k in range(nz * SIDE):
        to_core(k).wait_send()
    for zz in range(nz):
        to_y(zz).wait_send()
    for d in range(1, nz):
        to_z(d).wait_send()


def copy_kernel(*refs):
    for k in range(4):
        refs[4 + k][...] = refs[k][...]


def fused(n_inter, hidden_in, norm_gain, qkv_weight, attn_cotangent):
    toks, width = hidden_in.shape[1:]
    rows, cols = qkv_weight.shape
    nz = n_inter // (CORES * SIDE)
    chips = nz * SIDE
    freqs = rope_base ** (-np.arange(HD // 2, dtype=np.float32) / np.float32(HD // 2))
    angles = (np.arange(2 * toks, dtype=np.float32)[:, None] * freqs.astype(np.float32)[None, :]).astype(np.float32)
    cosine = np.concatenate([np.cos(angles)] * 2, axis=1).astype(np.float32)
    sine = np.concatenate([-np.sin(angles), np.sin(angles)], axis=1).astype(np.float32)
    bf, f32, dma = jnp.bfloat16, jnp.float32, pltpu.SemaphoreType.DMA
    vmem = pl.BlockSpec(memory_space=pltpu.VMEM)
    attn, gin, wg, gg = pl.pallas_call(
        functools.partial(fused_kernel, n_inter),
        out_shape=(
            jax.ShapeDtypeStruct((toks, HEADS * HD), bf),
            jax.ShapeDtypeStruct((toks, width), bf),
            jax.ShapeDtypeStruct((rows, cols), f32),
            jax.ShapeDtypeStruct((1, rows), f32),
        ),
        in_specs=[vmem] * 6,
        out_specs=(vmem,) * 4,
        scratch_shapes=[
            pltpu.VMEM((2 * n_inter, rows + GAIN_ROWS, cols), bf),
            pltpu.VMEM((toks, width), bf),
            pltpu.VMEM((2 * toks, width // 2), bf),
            pltpu.VMEM((2 * toks, 2 * HD), bf),
            pltpu.VMEM((2 * toks, 2 * HD), f32),
            pltpu.VMEM((toks, 2 * HD), f32),
            pltpu.VMEM((2 * toks, cols), bf),
            pltpu.VMEM((n_inter, rows, cols), bf),
            pltpu.VMEM((chips, rows, cols), bf),
            pltpu.VMEM((nz, rows, cols), bf),
            pltpu.VMEM((nz, rows, cols), bf),
            pltpu.VMEM((max(nz - 1, 1), rows, cols), bf),
            pltpu.VMEM((max(nz - 1, 1), rows, cols), bf),
            pltpu.VMEM((toks, cols), f32),
            dma((5, 2 * n_inter)), dma((2 * n_inter,)),
            dma((4,)), dma((4,)),
            dma((chips,)), dma((chips,)),
            dma((nz,)), dma((nz,)),
            dma((max(nz - 1, 1),)), dma((max(nz - 1, 1),)),
        ],
        compiler_params=pltpu.CompilerParams(
            collective_id=0, has_side_effects=True, vmem_limit_bytes=60 * 2**20
        ),
    )(hidden_in[0], norm_gain[None], qkv_weight, attn_cotangent[0], cosine, sine)
    outs = (attn, gin, wg, gg)
    attn, gin, wg, gg = pl.pallas_call(
        copy_kernel,
        out_shape=tuple(jax.ShapeDtypeStruct(o.shape, o.dtype) for o in outs),
        in_specs=[vmem] * 4,
        out_specs=(vmem,) * 4,
    )(*outs)
    return attn[None], gin[None], wg, gg[0]


def solution(mesh):
    n_inter, n_intra = mesh.shape["inter"], mesh.shape["intra"]

    def body(hidden_in, norm_gain, qkv_weight, attn_cotangent):
        fits = n_intra == 2 and n_inter % (CORES * SIDE) == 0
        fits = fits and qkv_weight.shape[0] == HD and hidden_in.shape[0] == 1
        fits = fits and hidden_in.shape[1] % HD == 0
        if fits:
            return fused(n_inter, hidden_in, norm_gain, qkv_weight, attn_cotangent)
        return local(hidden_in, norm_gain, qkv_weight, attn_cotangent)

    return jax.shard_map(
        body,
        mesh=mesh,
        in_specs=(
            P("inter", "intra", None),
            P(("inter", "intra")),
            P(("inter", "intra"), None),
            P("inter", "intra", None),
        ),
        out_specs=(
            P("inter", "intra", None),
            P("inter", "intra", None),
            P(("intra", "inter"), None),
            P(("intra", "inter")),
        ),
        check_vma=False,
    )
```

```python
import functools
import jax
import jax.numpy as jnp
import numpy as np
from jax import lax
from jax.experimental import pallas as pl
from jax.experimental.pallas import tpu as pltpu
from jax.sharding import PartitionSpec as P

HD = 128
HEADS = 4


eps_norm = 1e-05
rope_base = 500000.0


def rope_tables(positions, head_size):
    half_size = head_size // 2
    freqs = rope_base ** (-jnp.arange(half_size, dtype=jnp.float32) / half_size)
    angles = positions.astype(jnp.float32)[:, None] * freqs[None, :]
    return (jnp.cos(angles), jnp.sin(angles))


def rotate(values_in, cosine, sine):
    half_size = values_in.shape[-1] // 2
    first, second = (values_in[..., :half_size], values_in[..., half_size:])
    return jnp.concatenate(
        [first * cosine - second * sine, second * cosine + first * sine], axis=-1
    )


def unrotate(grad_out, cosine, sine):
    half_size = grad_out.shape[-1] // 2
    first, second = (grad_out[..., :half_size], grad_out[..., half_size:])
    return jnp.concatenate(
        [first * cosine + second * sine, second * cosine - first * sine], axis=-1
    )


def forward_fold(query_rows, row_pos):

    def forward_advance(carry, piece, start):
        row_top, row_total, weighted = carry
        key_part, value_part = piece
        scores = jnp.einsum("qd,kd->qk", query_rows, key_part, preferred_element_type=jnp.float32)
        key_pos = jnp.arange(key_part.shape[0], dtype=jnp.int32)
        allowed = key_pos[None, :] <= row_pos[:, None]
        scores = jnp.where(allowed, scores, -1e30)
        new_top = jnp.maximum(row_top, jnp.max(scores, axis=1))
        numbers = jnp.where(allowed, jnp.exp(scores - new_top[:, None]), 0.0)
        row_total = jnp.sum(numbers, axis=1)
        weighted = jnp.dot(
            numbers,
            value_part.astype(jnp.float32),
            precision=lax.Precision.HIGHEST,
            preferred_element_type=jnp.float32,
        )
        return (new_top, row_total, weighted)

    return forward_advance


def query_grad_fold(query_rows, row_pos, grad_flat, log_total, row_delta):

    def query_advance(grad_query, piece, start):
        key_part, value_part = piece
        scores = jnp.einsum("qd,kd->qk", query_rows, key_part, preferred_element_type=jnp.float32)
        key_pos = jnp.arange(key_part.shape[0], dtype=jnp.int32)
        allowed = key_pos[None, :] <= row_pos[:, None]
        probs = jnp.where(
            allowed, jnp.exp(jnp.where(allowed, scores, -1e30) - log_total[:, None]), 0.0
        )
        grad_probs = jnp.einsum(
            "qd,kd->qk", grad_flat, value_part, preferred_element_type=jnp.float32
        )
        grad_scores = (probs * (grad_probs - row_delta[:, None])).astype(jnp.bfloat16)
        return jnp.dot(grad_scores, key_part, preferred_element_type=jnp.float32)

    return query_advance


def key_grad_fold(key_rows, value_rows, key_pos, log_all, delta_all, heads_count):

    def key_advance(carry, piece, start):
        query_part, attn_grad_part = piece
        count = query_part.shape[0]
        scores = jnp.einsum("qd,kd->qk", query_part, key_rows, preferred_element_type=jnp.float32)
        query_pos = jnp.arange(count, dtype=jnp.int32) // heads_count
        allowed = key_pos[None, :] <= query_pos[:, None]
        probs = jnp.where(
            allowed, jnp.exp(jnp.where(allowed, scores, -1e30) - log_all[:, None]), 0.0
        )
        grad_values = jnp.einsum(
            "qk,qd->kd",
            probs.astype(jnp.bfloat16),
            attn_grad_part,
            preferred_element_type=jnp.float32,
        )
        grad_probs = jnp.einsum(
            "qd,kd->qk", attn_grad_part, value_rows, preferred_element_type=jnp.float32
        )
        grad_scores = (probs * (grad_probs - delta_all[:, None])).astype(jnp.bfloat16)
        grad_keys = jnp.einsum(
            "qk,qd->kd", grad_scores, query_part, preferred_element_type=jnp.float32
        )
        return (grad_keys, grad_values)

    return key_advance


def local(hidden_in, norm_gain, qkv_weight, attn_cotangent):
    rows_in = hidden_in[0]
    grad_attn = attn_cotangent[0]
    tokens_here = rows_in.shape[0]
    width = rows_in.shape[1]
    head_size = HD
    heads_count = HEADS
    qcols = heads_count * head_size
    scale = head_size ** (-0.5)
    weight_group, gain_group = (
        lax.all_gather(qkv_weight, "intra", axis=0, tiled=True),
        lax.all_gather(norm_gain, "intra", axis=0, tiled=True),
    )
    weight_full, gain_full = (
        lax.all_gather(weight_group, "inter", axis=0, tiled=True),
        lax.all_gather(gain_group, "inter", axis=0, tiled=True),
    )
    query_pos = lax.axis_index("intra") * tokens_here + jnp.arange(tokens_here, dtype=jnp.int32)
    row_pos = jnp.broadcast_to(query_pos[:, None], (tokens_here, heads_count)).reshape(
        tokens_here * heads_count
    )
    cosine, sine = rope_tables(query_pos, head_size)
    wide_rows = rows_in.astype(jnp.float32)
    inv_rms = lax.rsqrt(jnp.mean(wide_rows * wide_rows, axis=1, keepdims=True) + eps_norm)
    normed = (wide_rows * inv_rms * gain_full.astype(jnp.float32)[None, :]).astype(jnp.bfloat16)
    mixed = jnp.dot(normed, weight_full, preferred_element_type=jnp.float32)
    query_rows = (
        (
            rotate(
                mixed[:, :qcols].reshape(tokens_here, heads_count, head_size),
                cosine[:, None, :],
                sine[:, None, :],
            )
            * scale
        )
        .astype(jnp.bfloat16)
        .reshape(tokens_here * heads_count, head_size)
    )
    key_rows = rotate(mixed[:, qcols : qcols + head_size], cosine, sine).astype(jnp.bfloat16)
    value_rows = mixed[:, qcols + head_size :].astype(jnp.bfloat16)
    grad_flat = grad_attn.reshape(tokens_here * heads_count, head_size)
    flat_rows = tokens_here * heads_count
    forward_step = forward_fold(query_rows, row_pos)
    start_carry = (
        jnp.full((flat_rows,), -1e30, jnp.float32),
        jnp.zeros((flat_rows,), jnp.float32),
        jnp.zeros((flat_rows, head_size), jnp.float32),
    )
    row_top, row_total, weighted = forward_step(
        start_carry,
        (
            lax.all_gather(key_rows, "intra", axis=0, tiled=True),
            lax.all_gather(value_rows, "intra", axis=0, tiled=True),
        ),
        jnp.int32(0),
    )
    attn_flat = (weighted / row_total[:, None]).astype(jnp.bfloat16)
    log_total = row_top + jnp.log(row_total)
    row_delta = jnp.sum(grad_flat.astype(jnp.float32) * attn_flat.astype(jnp.float32), axis=1)
    query_step = query_grad_fold(query_rows, row_pos, grad_flat, log_total, row_delta)
    grad_query = query_step(
        jnp.zeros((flat_rows, head_size), jnp.float32),
        (
            lax.all_gather(key_rows, "intra", axis=0, tiled=True),
            lax.all_gather(value_rows, "intra", axis=0, tiled=True),
        ),
        jnp.int32(0),
    )
    log_all, delta_all = (
        lax.all_gather(log_total, "intra", axis=0, tiled=True),
        lax.all_gather(row_delta, "intra", axis=0, tiled=True),
    )
    key_step = key_grad_fold(key_rows, value_rows, query_pos, log_all, delta_all, heads_count)
    grad_keys, grad_values = key_step(
        (
            jnp.zeros((tokens_here, head_size), jnp.float32),
            jnp.zeros((tokens_here, head_size), jnp.float32),
        ),
        (
            lax.all_gather(query_rows, "intra", axis=0, tiled=True),
            lax.all_gather(grad_flat, "intra", axis=0, tiled=True),
        ),
        jnp.int32(0),
    )
    query_back = (
        unrotate(
            grad_query.reshape(tokens_here, heads_count, head_size),
            cosine[:, None, :],
            sine[:, None, :],
        )
        * scale
    ).reshape(tokens_here, qcols)
    grad_mixed = jnp.concatenate(
        [query_back, unrotate(grad_keys, cosine, sine), grad_values], axis=1
    ).astype(jnp.bfloat16)
    weight_back, gain_back = (weight_full, gain_full)
    gain_wide = gain_back.astype(jnp.float32)[None, :]
    grad_normed = jnp.einsum(
        "tc,dc->td", grad_mixed, weight_back, preferred_element_type=jnp.float32
    )
    inner = jnp.sum(grad_normed * gain_wide * wide_rows, axis=1, keepdims=True)
    grad_rows = (
        gain_wide * grad_normed * inv_rms - wide_rows * inv_rms**3 / width * inner
    ).astype(jnp.bfloat16)
    gain_term = jnp.sum(grad_normed * wide_rows * inv_rms, axis=0)
    normed_cols = lax.all_to_all(normed, "intra", split_axis=1, concat_axis=0, tiled=True)
    group_term = lax.dot_general(
        normed_cols,
        lax.all_gather(grad_mixed, "intra", axis=0, tiled=True),
        (((0,), (0,)), ((), ())),
        preferred_element_type=jnp.float32,
    )
    term_low = lax.optimization_barrier(group_term.astype(jnp.bfloat16))
    gain_sums = lax.psum_scatter(gain_term, "intra", scatter_dimension=0, tiled=True)
    weight_grad, gain_grad = (
        lax.psum_scatter(term_low.astype(jnp.float32), "inter", scatter_dimension=0, tiled=True),
        lax.psum_scatter(gain_sums, "inter", scatter_dimension=0, tiled=True),
    )
    return (attn_flat.reshape(tokens_here, qcols)[None], grad_rows[None], weight_grad, gain_grad)

MESH = pl.DeviceIdType.MESH
CORES = 2
SIDE = 2
GAIN_ROWS = 16


def nt_dot(a, b):
    return lax.dot_general(a, b, (((1,), (1,)), ((), ())), preferred_element_type=jnp.float32)


def tn_dot(a, b):
    return lax.dot_general(a, b, (((0,), (0,)), ((), ())), preferred_element_type=jnp.float32)


def nn_dot(a, b):
    return jnp.dot(a, b, preferred_element_type=jnp.float32)


def fused_kernel(
    n_inter,
    hid_ref, gain_ref, w_ref, ct_ref, cos_ref, sin_ref,
    attn_ref, gin_ref, wg_ref, gg_ref,
    wbuf, nrm, nbuf, kvbuf, gkv, gkv_out, gkv_in, gmbuf, tbuf, rs1, ybuf, rs2, zbuf, rs3, mix,
    ag_send, ag_recv, ex_send, ex_recv, c_send, c_recv, y_send, y_recv, z_send, z_recv,
):
    i = lax.axis_index("inter")
    x = lax.axis_index("intra")
    nz = n_inter // (CORES * SIDE)
    c = lax.rem(i, CORES)
    y = lax.rem(i // CORES, SIDE)
    z = i // (CORES * SIDE)
    toks, width = hid_ref.shape
    rows, cols = w_ref.shape
    half = width // 2
    qcols = HEADS * HD
    scale = HD ** (-0.5)

    def dev(zz, yy, cc, xx):
        return ((zz * SIDE + yy) * CORES + cc, xx)

    def slot(zz, yy, cc, xx):
        return ((zz * SIDE + yy) * CORES + cc) * 2 + xx

    x_peer = dev(z, y, c, 1 - x)
    y_peer = dev(z, 1 - y, c, x)
    c_peer = dev(z, y, 1 - c, x)

    def z_peer(zz):
        return dev(zz, y, c, x)

    own = slot(z, y, c, x)
    wbuf[own, :rows, :] = w_ref[...]
    wbuf[own, rows:, :HD] = jnp.broadcast_to(gain_ref[...], (GAIN_ROWS, HD))
    wbuf[own, rows:, HD:] = jnp.zeros((GAIN_ROWS, cols - HD), jnp.bfloat16)

    barrier = pltpu.get_barrier_semaphore()
    peers = [x_peer, y_peer, c_peer] + [z_peer(lax.rem(z + d, nz)) for d in range(1, nz)]
    for peer in peers:
        pl.semaphore_signal(barrier, inc=1, device_id=peer, device_id_type=MESH)
    pl.semaphore_wait(barrier, len(peers))

    targets = {
        0: x_peer,
        1: y_peer,
        2: z_peer(jnp.minimum(z + 1, nz - 1)),
        3: z_peer(jnp.maximum(z - 1, 0)),
        4: c_peer,
    }
    sent = []

    def ag(link, g):
        return pltpu.make_async_remote_copy(
            src_ref=wbuf.at[g], dst_ref=wbuf.at[g],
            send_sem=ag_send.at[link, g], recv_sem=ag_recv.at[g],
            device_id=targets[link], device_id_type=MESH,
        )

    def send(link, g, cond=None):
        sent.append((link, g, cond))
        if cond is None:
            ag(link, g).start()
        else:
            pl.when(cond)(lambda: ag(link, g).start())

    def arrive(g, cond=None):
        if cond is None:
            ag(0, g).wait_recv()
        else:
            pl.when(cond)(lambda: ag(0, g).wait_recv())

    def both(a, b):
        return b if a is None else jnp.logical_and(a, b)

    up, down = z < nz - 1, z > 0
    send(0, own)
    send(1, own)
    send(2, own, up)
    send(3, own, down)
    send(4, own)
    wide = hid_ref[...].astype(jnp.float32)
    inv = lax.rsqrt(jnp.mean(wide * wide, axis=1, keepdims=True) + eps_norm)
    mix[...] = jnp.zeros((toks, cols), jnp.float32)
    span = lambda g: pl.ds(pl.multiple_of(g * rows, rows), rows)

    def absorb(g):
        gain = wbuf[g, rows : rows + 1, :rows].astype(jnp.float32)
        part = (hid_ref[:, span(g)].astype(jnp.float32) * inv * gain).astype(jnp.bfloat16)
        nrm[:, span(g)] = part
        mix[...] += nn_dot(part, wbuf[g, :rows, :])

    def absorb_when(g, cond):
        if cond is None:
            absorb(g)
        else:
            pl.when(cond)(lambda: absorb(g))

    def sides(d):
        if d == 0:
            return [(z, None, None)]
        return [(z - d, z - d >= 0, 2), (z + d, z + d < nz, 3)]

    def onward(link):
        return up if link == 2 else down

    late = []

    def done(zz, yy, xx, ok):
        late.append((zz, yy, xx, ok))
        absorb_when(slot(zz, yy, c, xx), ok)

    def drain(count):
        for _ in range(min(count, len(late))):
            zz, yy, xx, ok = late.pop(0)
            g = slot(zz, yy, 1 - c, xx)
            arrive(g, ok)
            absorb_when(g, ok)

    def column(d):
        for zz, ok, link in sides(d):
            g = slot(zz, y, c, x)
            arrive(g, ok)
            send(link, g, both(ok, onward(link)))
            for k in (0, 1, 4):
                send(k, g, ok)
        for zz, ok, link in sides(d):
            done(zz, y, x, ok)

    direct = [d for d in range(nz) if d == 0 or d >= 3]

    def side(d):
        for zz, ok, link in sides(d):
            odd = lax.rem(zz + 2 * nz, 2) == 1
            g = slot(zz, y, c, 1 - x)
            arrive(g, ok)
            if d in direct:
                send(1, g, both(ok, odd))
            send(4, g, ok)
            g = slot(zz, 1 - y, c, x)
            arrive(g, ok)
            if d in direct:
                send(0, g, both(ok, jnp.logical_not(odd)))
            send(4, g, ok)
        for zz, ok, link in sides(d):
            done(zz, y, 1 - x, ok)
            done(zz, 1 - y, x, ok)

    def diagonal(d):
        for zz, ok, link in sides(d):
            g = slot(zz, 1 - y, c, 1 - x)
            arrive(g, ok)
            if d + 1 < nz and d + 1 not in direct:
                if d == 0:
                    send(2, g, up)
                    send(3, g, down)
                else:
                    send(link, g, both(ok, onward(link)))
            send(4, g, ok)
        for zz, ok, link in sides(d):
            done(zz, 1 - y, 1 - x, ok)

    done(z, y, x, None)
    steps = [(d * 3, column, d) for d in range(1, nz)]
    steps += [(d * 3 + 4, side, d) for d in range(nz)]
    steps += [(d * 3 + 8, diagonal, d) for d in range(nz)]
    for _, step, d in sorted(steps, key=lambda e: e[0]):
        waiting = len(late)
        step(d)
        drain(waiting)
    drain(len(late))
    acc = mix[...]

    cosine = cos_ref[pl.ds(pl.multiple_of(x * toks, toks), toks), :]
    sine = sin_ref[pl.ds(pl.multiple_of(x * toks, toks), toks), :]

    def rope(u):
        return u * cosine + pltpu.roll(u, HD // 2, 1) * sine

    def unrope(u):
        return u * cosine - pltpu.roll(u, HD // 2, 1) * sine

    here = pl.ds(pl.multiple_of(x * toks, toks), toks)
    there = pl.ds(pl.multiple_of((1 - x) * toks, toks), toks)

    def exchange(k, src, dst):
        return pltpu.make_async_remote_copy(
            src_ref=src, dst_ref=dst, send_sem=ex_send.at[k], recv_sem=ex_recv.at[k],
            device_id=x_peer, device_id_type=MESH,
        )

    kvbuf[here, :HD] = rope(acc[:, qcols : qcols + HD]).astype(jnp.bfloat16)
    kvbuf[here, HD:] = acc[:, qcols + HD :].astype(jnp.bfloat16)
    query = [(rope(acc[:, h * HD : (h + 1) * HD]) * scale).astype(jnp.bfloat16) for h in range(HEADS)]
    query = jnp.concatenate(query, axis=0)
    kv_copy = exchange(0, kvbuf.at[here], kvbuf.at[here])
    kv_copy.start()
    keep = pl.ds(pl.multiple_of(x * half, half), half)
    part = half // 2
    norm_copy, norm_rest = [
        exchange(
            k,
            nrm.at[:, pl.ds(pl.multiple_of((1 - x) * half + first, part), part)],
            nbuf.at[here, first : first + part],
        )
        for k, first in ((1, 0), (4, part))
    ]
    norm_copy.start()
    nbuf[here, :] = nrm[:, keep]
    kv_copy.wait()

    flat = HEADS * toks
    keys, values = kvbuf[:, :HD], kvbuf[:, HD:]
    row_pos = x * toks + lax.rem(lax.broadcasted_iota(jnp.int32, (flat, 2 * toks), 0), toks)
    allowed = lax.broadcasted_iota(jnp.int32, (flat, 2 * toks), 1) <= row_pos
    scores = jnp.where(allowed, nt_dot(query, keys), -1e30)
    top = jnp.max(scores, axis=1, keepdims=True)
    numbers = jnp.where(allowed, jnp.exp(scores - top), 0.0)
    total = jnp.sum(numbers, axis=1, keepdims=True)
    high = numbers.astype(jnp.bfloat16)
    low = (numbers - high.astype(jnp.float32)).astype(jnp.bfloat16)
    attn = ((nn_dot(high, values) + nn_dot(low, values)) / total).astype(jnp.bfloat16)
    for h in range(HEADS):
        attn_ref[:, h * HD : (h + 1) * HD] = attn[h * toks : (h + 1) * toks]
    grad = jnp.concatenate([ct_ref[:, h * HD : (h + 1) * HD] for h in range(HEADS)], axis=0)
    delta = jnp.sum(grad.astype(jnp.float32) * attn.astype(jnp.float32), axis=1, keepdims=True)
    probs = numbers / total
    grad_scores = (probs * (nt_dot(grad, values) - delta)).astype(jnp.bfloat16)
    gkv[:, :HD] = tn_dot(grad_scores, query)
    gkv[:, HD:] = tn_dot(probs.astype(jnp.bfloat16), grad)
    gkv_out[...] = gkv[there, :].astype(jnp.bfloat16)
    gkv_copy = exchange(2, gkv_out, gkv_in)
    gkv_copy.start()
    norm_rest.start()
    grad_query = nn_dot(grad_scores, keys)
    for h in range(HEADS):
        gmbuf[here, h * HD : (h + 1) * HD] = (
            unrope(grad_query[h * toks : (h + 1) * toks]) * scale
        ).astype(jnp.bfloat16)
    gkv_copy.wait()
    own_kv = gkv[here, :] + gkv_in[...].astype(jnp.float32)
    gmbuf[here, qcols : qcols + HD] = unrope(own_kv[:, :HD]).astype(jnp.bfloat16)
    gmbuf[here, qcols + HD :] = own_kv[:, HD:].astype(jnp.bfloat16)
    gm_copy = exchange(3, gmbuf.at[here], gmbuf.at[here])
    gm_copy.start()

    gm = gmbuf[here, :]
    inner = jnp.sum(gm.astype(jnp.float32) * mix[...], axis=1, keepdims=True)
    back = inner * (inv * inv / width)

    def grad_rows(first, last):
        for g in range(first, last):
            lanes = slice(g * rows, (g + 1) * rows)
            gain = wbuf[g, rows : rows + 1, :rows].astype(jnp.float32)
            part = nt_dot(gm, wbuf[g, :rows, :])
            gin_ref[:, lanes] = (
                gain * part * inv - hid_ref[:, lanes].astype(jnp.float32) * back
            ).astype(jnp.bfloat16)

    pieces = nz + 1
    marks = [2 * n_inter * k // pieces for k in range(pieces + 1)]
    grad_rows(marks[0], marks[1])
    norm_copy.wait()
    norm_rest.wait()
    gm_copy.wait()

    both_gm = gmbuf[...]

    def term(k, cc):
        j = k * CORES + cc
        lanes = pl.ds(pl.multiple_of(j * rows, rows), rows)
        tbuf[j] = tn_dot(nbuf[:, lanes], both_gm).astype(jnp.bfloat16)

    def to_core(k):
        return pltpu.make_async_remote_copy(
            src_ref=tbuf.at[k * CORES + 1 - c], dst_ref=rs1.at[k],
            send_sem=c_send.at[k], recv_sem=c_recv.at[k], device_id=c_peer, device_id_type=MESH,
        )

    def to_y(zz):
        return pltpu.make_async_remote_copy(
            src_ref=ybuf.at[zz], dst_ref=rs2.at[zz],
            send_sem=y_send.at[zz], recv_sem=y_recv.at[zz], device_id=y_peer, device_id_type=MESH,
        )

    def to_z(d):
        return pltpu.make_async_remote_copy(
            src_ref=zbuf.at[d - 1], dst_ref=rs3.at[d - 1],
            send_sem=z_send.at[d - 1], recv_sem=z_recv.at[d - 1],
            device_id=z_peer(lax.rem(z + d, nz)), device_id_type=MESH,
        )

    order = [(d, lax.rem(z + d, nz)) for d in list(range(1, nz)) + [0]]

    def core_sum(k):
        to_core(k).wait_recv()
        return tbuf[k * CORES + c].astype(jnp.float32) + rs1[k].astype(jnp.float32)

    def to_y_side(zz):
        ybuf[zz] = core_sum(zz * SIDE + 1 - y).astype(jnp.bfloat16)
        to_y(zz).start()

    last = None
    for d, zz in order:
        k = zz * SIDE + 1 - y
        term(k, 1 - c)
        to_core(k).start()
        term(k, c)
        if last is not None:
            to_y_side(last)
        last = zz
    for n, (d, zz) in enumerate(order):
        k = zz * SIDE + y
        term(k, 1 - c)
        to_core(k).start()
        if n == 0:
            to_y_side(last)
        term(k, c)
    for n, (d, zz) in enumerate(order):
        grad_rows(marks[n + 1], marks[n + 2])
        part = core_sum(zz * SIDE + y)
        to_y(zz).wait_recv()
        part = part + rs2[zz].astype(jnp.float32)
        if d:
            zbuf[d - 1] = part.astype(jnp.bfloat16)
            to_z(d).start()
        else:
            wg_ref[...] = part
    result = wg_ref[...]
    for d in range(1, nz):
        to_z(d).wait_recv()
        result = result + rs3[d - 1].astype(jnp.float32)
    wg_ref[...] = result
    block = x * n_inter + i
    mixed_sum = wbuf[block, :rows, :].astype(jnp.float32) * result
    lanes_sum = mixed_sum[:, :HD]
    for k in range(1, cols // HD):
        lanes_sum = lanes_sum + mixed_sum[:, k * HD : (k + 1) * HD]
    gain = wbuf[block, rows : rows + 1, :rows].astype(jnp.float32)
    gg_ref[...] = jnp.sum(lanes_sum.T, axis=0, keepdims=True) / gain

    for link, g, cond in sent:
        if cond is None:
            ag(link, g).wait_send()
        else:
            pl.when(cond)(functools.partial(lambda l, s: ag(l, s).wait_send(), link, g))
    for k in range(nz * SIDE):
        to_core(k).wait_send()
    for zz in range(nz):
        to_y(zz).wait_send()
    for d in range(1, nz):
        to_z(d).wait_send()


def copy_kernel(*refs):
    for k in range(4):
        refs[4 + k][...] = refs[k][...]


def fused(n_inter, hidden_in, norm_gain, qkv_weight, attn_cotangent):
    toks, width = hidden_in.shape[1:]
    rows, cols = qkv_weight.shape
    nz = n_inter // (CORES * SIDE)
    chips = nz * SIDE
    freqs = rope_base ** (-np.arange(HD // 2, dtype=np.float32) / np.float32(HD // 2))
    angles = (np.arange(2 * toks, dtype=np.float32)[:, None] * freqs.astype(np.float32)[None, :]).astype(np.float32)
    cosine = np.concatenate([np.cos(angles)] * 2, axis=1).astype(np.float32)
    sine = np.concatenate([-np.sin(angles), np.sin(angles)], axis=1).astype(np.float32)
    bf, f32, dma = jnp.bfloat16, jnp.float32, pltpu.SemaphoreType.DMA
    vmem = pl.BlockSpec(memory_space=pltpu.VMEM)
    attn, gin, wg, gg = pl.pallas_call(
        functools.partial(fused_kernel, n_inter),
        out_shape=(
            jax.ShapeDtypeStruct((toks, HEADS * HD), bf),
            jax.ShapeDtypeStruct((toks, width), bf),
            jax.ShapeDtypeStruct((rows, cols), f32),
            jax.ShapeDtypeStruct((1, rows), f32),
        ),
        in_specs=[vmem] * 6,
        out_specs=(vmem,) * 4,
        scratch_shapes=[
            pltpu.VMEM((2 * n_inter, rows + GAIN_ROWS, cols), bf),
            pltpu.VMEM((toks, width), bf),
            pltpu.VMEM((2 * toks, width // 2), bf),
            pltpu.VMEM((2 * toks, 2 * HD), bf),
            pltpu.VMEM((2 * toks, 2 * HD), f32),
            pltpu.VMEM((toks, 2 * HD), bf),
            pltpu.VMEM((toks, 2 * HD), bf),
            pltpu.VMEM((2 * toks, cols), bf),
            pltpu.VMEM((n_inter, rows, cols), bf),
            pltpu.VMEM((chips, rows, cols), bf),
            pltpu.VMEM((nz, rows, cols), bf),
            pltpu.VMEM((nz, rows, cols), bf),
            pltpu.VMEM((max(nz - 1, 1), rows, cols), bf),
            pltpu.VMEM((max(nz - 1, 1), rows, cols), bf),
            pltpu.VMEM((toks, cols), f32),
            dma((5, 2 * n_inter)), dma((2 * n_inter,)),
            dma((5,)), dma((5,)),
            dma((chips,)), dma((chips,)),
            dma((nz,)), dma((nz,)),
            dma((max(nz - 1, 1),)), dma((max(nz - 1, 1),)),
        ],
        compiler_params=pltpu.CompilerParams(
            collective_id=0, has_side_effects=True, vmem_limit_bytes=60 * 2**20
        ),
    )(hidden_in[0], norm_gain[None], qkv_weight, attn_cotangent[0], cosine, sine)
    outs = (attn, gin, wg, gg)
    attn, gin, wg, gg = pl.pallas_call(
        copy_kernel,
        out_shape=tuple(jax.ShapeDtypeStruct(o.shape, o.dtype) for o in outs),
        in_specs=[vmem] * 4,
        out_specs=(vmem,) * 4,
    )(*outs)
    return attn[None], gin[None], wg, gg[0]


def solution(mesh):
    n_inter, n_intra = mesh.shape["inter"], mesh.shape["intra"]

    def body(hidden_in, norm_gain, qkv_weight, attn_cotangent):
        fits = n_intra == 2 and n_inter % (CORES * SIDE) == 0
        fits = fits and qkv_weight.shape[0] == HD and hidden_in.shape[0] == 1
        fits = fits and hidden_in.shape[1] % HD == 0
        if fits:
            return fused(n_inter, hidden_in, norm_gain, qkv_weight, attn_cotangent)
        return local(hidden_in, norm_gain, qkv_weight, attn_cotangent)

    return jax.shard_map(
        body,
        mesh=mesh,
        in_specs=(
            P("inter", "intra", None),
            P(("inter", "intra")),
            P(("inter", "intra"), None),
            P("inter", "intra", None),
        ),
        out_specs=(
            P("inter", "intra", None),
            P("inter", "intra", None),
            P(("intra", "inter"), None),
            P(("intra", "inter")),
        ),
        check_vma=False,
    )
```
